32 devices in a mesh: frame: 32 (over z, y, x, core), segment: 1.
Axes of the slice: x: 2, y: 2, z: 4, core: 2. Of those that a mesh axis runs over, the one named last changes fastest.
Arguments:
- state: bfloat16 [1, 1024, 3072], P('segment', 'frame'), may hold values from -6 to 6
- modulation: float32 [1, 32, 7, 3072], P('segment'), may hold values from -3 to 3
- noise_level: int32 [4], replicated, may hold values from 0 to 31
- frame_mask: int32 [4, 4], replicated, may hold values from 0 to 1, as said below
- offset: int32 [1], replicated, may hold values from 1 to 3
Outputs:
- next_state: bfloat16 [1, 1024, 3072], P('segment', 'frame')
The draws below stay inside these ranges and needn't reach their ends.
Inputs may be any that keep to these rules, and one draw needn't show every extreme that they name: frame_mask[i, i] is 1 and frame_mask[i, j] is 0 for j > i.
All inputs are finite; a program needn't handle non-finite values.
Results may differ from the reference program's by a relative error of at most 0.017.
Values may be sent and summed in bfloat16 or wider, within the bound.
A program may use at most 128 MiB of HBM per device.

```python
import math
import jax
import jax.numpy as jnp
from jax import lax

D = 3072
HEADS = 24
HEAD = 128
LEVELS = 32
FRAME_TOK = 256
FRAMES = 4
TOKENS = 1024
N_SEGMENT = 1


def draw_frame_mask(key, part):
    frames_all = TOKENS // FRAME_TOK
    picks = jax.random.randint(jax.random.fold_in(key, 17), (frames_all, frames_all), 0, 4)
    row_ids = jnp.arange(frames_all, dtype=jnp.int32)[:, None]
    col_ids = jnp.arange(frames_all, dtype=jnp.int32)[None, :]
    earlier = jnp.where(picks > 0, 1, 0)
    return jnp.where(row_ids > col_ids, earlier, jnp.where(row_ids == col_ids, 1, 0)).astype(jnp.int32)


def draw_state(key, part):
    frames_all = TOKENS // FRAME_TOK
    background_share = 0.3
    carry_rate = 0.4 ** (1.0 / frames_all)
    fresh = jax.random.normal(jax.random.fold_in(key, 5), (N_SEGMENT, frames_all, FRAME_TOK * D), jnp.float32)
    frame_ids = jnp.arange(frames_all, dtype=jnp.int32)
    lag = frame_ids[:, None] - frame_ids[None, :]
    lag_float = jnp.maximum(lag, 0).astype(jnp.float32)
    entry_scale = jnp.where(frame_ids[None, :] == 0, 1.0, math.sqrt(1.0 - carry_rate * carry_rate))
    mixing = jnp.where(lag >= 0, jnp.power(jnp.float32(carry_rate), lag_float) * entry_scale, 0.0).astype(jnp.float32)
    carried = jnp.einsum('fg,sgc->sfc', mixing, fresh, precision=lax.Precision.HIGHEST)
    carried = carried.reshape(N_SEGMENT, frames_all, FRAME_TOK, D)
    backdrop = jax.random.normal(jax.random.fold_in(key, 9), (N_SEGMENT, D), jnp.float32)
    backdrop = backdrop / jnp.sqrt(jnp.mean(backdrop * backdrop, axis=-1, keepdims=True))
    framed = math.sqrt(background_share) * backdrop[:, None, None, :] + math.sqrt(1.0 - background_share) * carried
    noise_field = framed.reshape(N_SEGMENT, TOKENS, D)
    return jnp.clip(noise_field, -6.0, 6.0).astype(jnp.bfloat16)


def with_ends(drawn, key, low, high):
    shape = drawn.shape
    spot = [jax.random.randint(jax.random.fold_in(key, axis), (), 0, shape[axis]) for axis in range(len(shape))]
    drawn = drawn.at[tuple(spot)].set(low)
    longest = shape.index(max(shape))
    spot[longest] = (spot[longest] + 1) % shape[longest]
    return drawn.at[tuple(spot)].set(high)


def gaussian(stream_key, extent, spread, reach, kind=jnp.bfloat16):
    drawn = jax.random.normal(stream_key, extent, jnp.float32) * spread
    return jnp.minimum(jnp.maximum(drawn, -reach), reach).astype(kind)


def setup_inputs(seed: int = 0) -> dict:
    keys = jax.random.split(jax.random.key(seed), 6)
    return {
        "state": draw_state(jax.random.fold_in(keys[5], 71), 0),
        "modulation": gaussian(keys[1], (N_SEGMENT, LEVELS, 7, D), 0.5, 3.0, jnp.float32),
        "noise_level": with_ends(jax.random.randint(keys[2], (FRAMES,), 0, LEVELS), jax.random.fold_in(keys[2], 1), 0, LEVELS - 1).astype(jnp.int32),
        "frame_mask": draw_frame_mask(jax.random.fold_in(keys[5], 71), 0),
        "offset": jax.random.randint(keys[4], (1,), 1, FRAMES).astype(jnp.int32),
    }


epsilon = 1e-06

def normalize(values):
    widened = values.astype(jnp.float32)
    square_mean = lax.optimization_barrier(jnp.mean(widened * widened, axis=-1, keepdims=True))
    return (widened * lax.rsqrt(square_mean + epsilon)).astype(jnp.bfloat16)

def modulate(normed, modifiers, column):
    scaled = normed.astype(jnp.float32) * (1.0 + modifiers[:, column]) + modifiers[:, column + 1]
    return scaled.astype(jnp.bfloat16)

def section(hidden, level_table, noise_level, frame_mask):
    tokens_all = hidden.shape[0]
    row_frames = jnp.arange(tokens_all, dtype=jnp.int32) // FRAME_TOK
    modifiers = level_table[noise_level[row_frames]]
    normed = normalize(hidden)
    queries = modulate(normed, modifiers, 0)
    keys_all = modulate(normed, modifiers, 2)
    values_all = modulate(normed, modifiers, 4)
    allowed = frame_mask[row_frames][:, row_frames] == 1
    scale_factor = 1.0 / math.sqrt(HEAD)

    def split_heads(rows):
        return jnp.transpose(rows.reshape(tokens_all, HEADS, HEAD), (1, 0, 2))

    def per_head(stacked):
        query_head, key_head, value_head = stacked
        scores = jnp.dot(query_head, key_head.T, preferred_element_type=jnp.float32) * scale_factor
        scores = jnp.where(allowed, scores, jnp.float32(-1e+30))
        row_max = lax.optimization_barrier(jnp.max(scores, axis=-1, keepdims=True))
        weights = jnp.where(allowed, jnp.exp(scores - row_max), jnp.float32(0.0)).astype(jnp.bfloat16)
        summed = jnp.dot(weights, value_head, preferred_element_type=jnp.float32)
        denominator = lax.optimization_barrier(jnp.sum(weights.astype(jnp.float32), axis=-1, keepdims=True))
        return (summed / denominator).astype(jnp.bfloat16)
    heads_out = lax.map(per_head, (split_heads(queries), split_heads(keys_all), split_heads(values_all)))
    attention = jnp.transpose(heads_out, (1, 0, 2)).reshape(tokens_all, HEADS * HEAD)
    updated = hidden.astype(jnp.float32) + modifiers[:, 6] * attention.astype(jnp.float32)
    return updated.astype(jnp.bfloat16)

def reference(state, modulation, noise_level, frame_mask, offset):
    outputs = [section(state[segment_num], modulation[segment_num], noise_level, frame_mask) for segment_num in range(N_SEGMENT)]
    wrapped = jnp.roll(outputs[-1], -offset[0] * FRAME_TOK, axis=0)
    return jnp.stack([wrapped] + outputs[:-1])
```

```python
import functools
import math

import jax
import jax.numpy as jnp
from jax import lax
from jax.experimental import pallas as pl
from jax.experimental.pallas import tpu as pltpu
from jax.sharding import PartitionSpec as P

HEAD = 128
FRAME_TOK = 256

epsilon = 1e-06
negative = -1e30


def kernel(
    devices,
    segments,
    heads,
    frames,
    rows,
    level_ref,
    mask_ref,
    offset_ref,
    state_ref,
    mod_ref,
    out_ref,
    local,
    gathered,
    scale_out,
    scales,
    mods,
    normed,
    keys,
    values,
    outgoing,
    local_sem,
    mod_sem,
    state_send,
    state_recv,
    scale_send,
    scale_recv,
    out_send,
    out_recv,
):
    me = lax.axis_index("frame")
    segment = lax.axis_index("segment")
    span = FRAME_TOK // rows
    width = heads * HEAD
    my_head = lax.div(me * heads + devices - 1, devices)
    owner = lax.div(my_head * devices, heads) == me
    my_columns = pl.multiple_of(my_head * HEAD, HEAD)
    my_frame = lax.div(me, span)
    my_row = pl.multiple_of(lax.rem(me, span) * rows, rows)

    fetch = pltpu.make_async_copy(state_ref.at[0], local, local_sem)
    fetch.start()

    def state_copy(head):
        target = lax.div(head * devices, heads)
        columns = pl.ds(pl.multiple_of(head * HEAD, HEAD), HEAD)
        return target, pltpu.make_async_remote_copy(
            src_ref=state_ref.at[0, :, columns],
            dst_ref=gathered.at[my_frame, pl.ds(my_row, rows), :],
            send_sem=state_send.at[head],
            recv_sem=state_recv.at[my_frame],
            device_id={"frame": target},
            device_id_type=pl.DeviceIdType.MESH,
        )

    def scale_copy(head):
        target = lax.div(head * devices, heads)
        return target, pltpu.make_async_remote_copy(
            src_ref=scale_out,
            dst_ref=scales.at[me],
            send_sem=scale_send.at[head],
            recv_sem=scale_recv,
            device_id={"frame": target},
            device_id_type=pl.DeviceIdType.MESH,
        )

    first_head = lax.div(me * heads, devices)

    def for_heads(make, act):
        def step(index, carry):
            head = lax.rem(first_head + index, heads)
            target, copy = make(head)

            @pl.when(target != me)
            def _():
                act(copy)

            return carry

        lax.fori_loop(0, heads, step, 0)

    for_heads(state_copy, lambda copy: copy.start())

    @pl.when(owner)
    def _():
        pltpu.make_async_copy(
            mod_ref.at[0, :, :, pl.ds(my_columns, HEAD)], mods, mod_sem
        ).start()
        pltpu.make_async_copy(
            state_ref.at[0, :, pl.ds(my_columns, HEAD)],
            gathered.at[my_frame, pl.ds(my_row, rows), :],
            state_recv.at[my_frame],
        ).start()

    fetch.wait()
    widened = local[...].astype(jnp.float32)
    square_mean = jnp.sum(widened * widened, axis=-1, keepdims=True) * (1.0 / width)
    factor = lax.rsqrt(square_mean + epsilon)
    diagonal = lax.broadcasted_iota(jnp.int32, (rows, HEAD), 0) == lax.broadcasted_iota(
        jnp.int32, (rows, HEAD), 1
    )
    scale_out[...] = jnp.sum(
        jnp.where(diagonal, factor, 0.0), axis=0, keepdims=True
    )
    for_heads(scale_copy, lambda copy: copy.start())

    nxt = lax.rem(segment + 1, segments)

    def out_copy(place, part):
        target = place * span + part
        return target, pltpu.make_async_remote_copy(
            src_ref=outgoing.at[place, pl.ds(pl.multiple_of(part * rows, rows), rows), :],
            dst_ref=out_ref.at[0, :, pl.ds(my_columns, HEAD)],
            send_sem=out_send.at[target],
            recv_sem=out_recv,
            device_id={"frame": target, "segment": nxt},
            device_id_type=pl.DeviceIdType.MESH,
        )

    def send_place(place, begin):
        def step(part, carry):
            target, copy = out_copy(place, part)
            remote = jnp.logical_or(target != me, nxt != segment)

            @pl.when(remote)
            def _():
                if begin:
                    copy.start()
                else:
                    copy.wait_send()

            if begin:
                @pl.when(jnp.logical_not(remote))
                def _():
                    pltpu.make_async_copy(
                        outgoing.at[place, pl.ds(pl.multiple_of(part * rows, rows), rows), :],
                        out_ref.at[0, :, pl.ds(my_columns, HEAD)],
                        out_recv,
                    ).start()

            return carry

        lax.fori_loop(0, span, step, 0)

    @pl.when(owner)
    def _():
        pltpu.make_async_copy(scale_out, scales.at[me], scale_recv).start()
        values[:, HEAD:] = jnp.ones((frames * FRAME_TOK, HEAD), jnp.bfloat16)
        pltpu.make_async_copy(
            mod_ref.at[0, :, :, pl.ds(my_columns, HEAD)], mods, mod_sem
        ).wait()
        pltpu.make_async_copy(scales, scales, scale_recv).wait()
        for frame in range(frames):
            pltpu.make_async_copy(
                gathered.at[frame], gathered.at[frame], state_recv.at[frame]
            ).wait()
            row_mods = mods[level_ref[frame]]
            for part in range(span):
                column = jnp.sum(
                    jnp.where(diagonal, scales[frame * span + part], 0.0),
                    axis=1,
                    keepdims=True,
                )
                inner = slice(part * rows, (part + 1) * rows)
                outer = slice(frame * FRAME_TOK + part * rows, frame * FRAME_TOK + (part + 1) * rows)
                scaled = (
                    gathered[frame, inner, :].astype(jnp.float32) * column
                ).astype(jnp.bfloat16)
                normed[frame, inner, :] = scaled
                wide = scaled.astype(jnp.float32)
                keys[outer, :] = (
                    wide * (1.0 + row_mods[2:3]) + row_mods[3:4]
                ).astype(jnp.bfloat16)
                values[outer, :HEAD] = (
                    wide * (1.0 + row_mods[4:5]) + row_mods[5:6]
                ).astype(jnp.bfloat16)

        shift = jnp.where(segment == segments - 1, offset_ref[0], 0)
        for place in range(frames):
            frame = lax.rem(place + shift, frames)
            row_mods = mods[level_ref[frame]]
            queries = (
                normed[frame].astype(jnp.float32) * (1.0 + row_mods[0:1]) + row_mods[1:2]
            ).astype(jnp.bfloat16)
            bias = jnp.concatenate(
                [
                    jnp.full(
                        (1, FRAME_TOK),
                        jnp.where(mask_ref[frame, other] == 1, 0.0, negative),
                        jnp.float32,
                    )
                    for other in range(frames)
                ],
                axis=1,
            )
            scores = lax.dot_general(
                queries,
                keys[...],
                (((1,), (1,)), ((), ())),
                preferred_element_type=jnp.float32,
            )
            scores = scores * (1.0 / math.sqrt(HEAD)) + bias
            weights = jnp.exp(scores - jnp.max(scores, axis=-1, keepdims=True)).astype(
                jnp.bfloat16
            )
            summed = jnp.dot(weights, values[...], preferred_element_type=jnp.float32)
            attention = (summed[:, :HEAD] / summed[:, HEAD:]).astype(jnp.bfloat16)
            outgoing[place] = (
                gathered[frame].astype(jnp.float32)
                + row_mods[6:7] * attention.astype(jnp.float32)
            ).astype(jnp.bfloat16)
            send_place(place, True)

    for_heads(state_copy, lambda copy: copy.wait_send())
    for_heads(scale_copy, lambda copy: copy.wait_send())

    @pl.when(owner)
    def _():
        for place in range(frames):
            send_place(place, False)

    pltpu.make_async_copy(out_ref, out_ref, out_recv).wait()


def body(state, modulation, noise_level, frame_mask, offset):
    _, rows, width = state.shape
    _, levels, kinds, _ = modulation.shape
    devices = lax.axis_size("frame")
    segments = lax.axis_size("segment")
    heads = width // HEAD
    frames = devices * rows // FRAME_TOK
    tokens = devices * rows
    smem = pl.BlockSpec(memory_space=pltpu.SMEM)
    hbm = pl.BlockSpec(memory_space=pl.ANY)
    return pl.pallas_call(
        functools.partial(kernel, devices, segments, heads, frames, rows),
        out_shape=jax.ShapeDtypeStruct(state.shape, jnp.bfloat16),
        in_specs=[smem, smem, smem, hbm, hbm],
        out_specs=pl.BlockSpec(memory_space=pltpu.VMEM),
        scratch_shapes=[
            pltpu.VMEM((rows, width), jnp.bfloat16),
            pltpu.VMEM((frames, FRAME_TOK, HEAD), jnp.bfloat16),
            pltpu.VMEM((1, HEAD), jnp.float32),
            pltpu.VMEM((devices, 1, HEAD), jnp.float32),
            pltpu.VMEM((levels, kinds, HEAD), jnp.float32),
            pltpu.VMEM((frames, FRAME_TOK, HEAD), jnp.bfloat16),
            pltpu.VMEM((tokens, HEAD), jnp.bfloat16),
            pltpu.VMEM((tokens, 2 * HEAD), jnp.bfloat16),
            pltpu.VMEM((frames, FRAME_TOK, HEAD), jnp.bfloat16),
            pltpu.SemaphoreType.DMA,
            pltpu.SemaphoreType.DMA,
            pltpu.SemaphoreType.DMA((heads,)),
            pltpu.SemaphoreType.DMA((frames,)),
            pltpu.SemaphoreType.DMA((heads,)),
            pltpu.SemaphoreType.DMA,
            pltpu.SemaphoreType.DMA((devices,)),
            pltpu.SemaphoreType.DMA,
        ],
        compiler_params=pltpu.CompilerParams(has_side_effects=True),
        name="denoise",
    )(noise_level, frame_mask, offset, state, modulation)


def solution(mesh):
    return jax.shard_map(
        body,
        mesh=mesh,
        in_specs=(P("segment", "frame", None), P("segment", None, None, None), P(), P(), P()),
        out_specs=P("segment", "frame", None),
        check_vma=False,
    )
```

```python
import functools
import math

import jax
import jax.numpy as jnp
from jax import lax
from jax.experimental import pallas as pl
from jax.experimental.pallas import tpu as pltpu
from jax.sharding import PartitionSpec as P

HEAD = 128
FRAME_TOK = 256

epsilon = 1e-06
negative = -1e30


def kernel(
    devices,
    segments,
    heads,
    frames,
    rows,
    level_ref,
    mask_ref,
    offset_ref,
    state_ref,
    mod_ref,
    out_ref,
    local,
    gathered,
    scale_out,
    scales,
    mods,
    normed,
    keys,
    values,
    outgoing,
    local_sem,
    mod_sem,
    state_send,
    state_recv,
    scale_send,
    scale_recv,
    out_send,
    out_recv,
):
    me = lax.axis_index("frame")
    segment = lax.axis_index("segment")
    span = FRAME_TOK // rows
    width = heads * HEAD
    my_head = lax.min(me, heads - 1)
    owner = me < heads
    my_columns = pl.multiple_of(my_head * HEAD, HEAD)
    my_frame = lax.div(me, span)
    my_row = pl.multiple_of(lax.rem(me, span) * rows, rows)

    nxt = lax.rem(segment + 1, segments)
    barrier = pltpu.get_barrier_semaphore()

    def greet(peer, peer_segment):
        pl.semaphore_signal(
            barrier,
            inc=1,
            device_id={"frame": peer, "segment": peer_segment},
            device_id_type=pl.DeviceIdType.MESH,
        )

    def greet_reader(index, carry):
        greet(lax.rem(me + index, devices), segment)
        return carry

    def greet_writer(head, carry):
        greet(head, lax.rem(segment + segments - 1, segments))
        return carry

    fetch = pltpu.make_async_copy(state_ref.at[0], local, local_sem)
    fetch.start()

    @pl.when(owner)
    def _():
        lax.fori_loop(1, devices, greet_reader, 0)
        pltpu.make_async_copy(
            mod_ref.at[0, :, :, pl.ds(my_columns, HEAD)], mods, mod_sem
        ).start()

    if segments > 1:
        lax.fori_loop(0, heads, greet_writer, 0)

    fetch.wait()
    widened = local[...].astype(jnp.float32)
    square_mean = jnp.sum(widened * widened, axis=-1, keepdims=True) * (1.0 / width)
    factor = lax.rsqrt(square_mean + epsilon)
    diagonal = lax.broadcasted_iota(jnp.int32, (rows, HEAD), 0) == lax.broadcasted_iota(
        jnp.int32, (rows, HEAD), 1
    )
    scale_out[...] = jnp.sum(
        jnp.where(diagonal, factor, 0.0), axis=0, keepdims=True
    )

    greetings = heads - jnp.where(owner, 1, 0)
    if segments > 1:
        greetings += jnp.where(owner, devices, 0)
    pl.semaphore_wait(barrier, greetings)

    def state_copy(head):
        columns = pl.ds(pl.multiple_of(head * HEAD, HEAD), HEAD)
        return pltpu.make_async_remote_copy(
            src_ref=local.at[:, columns],
            dst_ref=gathered.at[my_frame, pl.ds(my_row, rows), :],
            send_sem=state_send.at[head],
            recv_sem=state_recv.at[my_frame],
            device_id={"frame": head},
            device_id_type=pl.DeviceIdType.MESH,
        )

    def scale_copy(head):
        return pltpu.make_async_remote_copy(
            src_ref=scale_out,
            dst_ref=scales.at[me],
            send_sem=scale_send.at[head],
            recv_sem=scale_recv.at[my_frame],
            device_id={"frame": head},
            device_id_type=pl.DeviceIdType.MESH,
        )

    def for_heads(act):
        def step(index, carry):
            head = lax.rem(me + index, heads)

            @pl.when(head != me)
            def _():
                act(head)

            return carry

        lax.fori_loop(0, heads, step, 0)

    def send_rows(head):
        state_copy(head).start()
        scale_copy(head).start()

    def end_rows(head):
        state_copy(head).wait_send()
        scale_copy(head).wait_send()

    for_heads(send_rows)

    @pl.when(owner)
    def _():
        pltpu.make_async_copy(
            local.at[:, pl.ds(my_columns, HEAD)],
            gathered.at[my_frame, pl.ds(my_row, rows), :],
            state_recv.at[my_frame],
        ).start()
        pltpu.make_async_copy(scale_out, scales.at[me], scale_recv.at[my_frame]).start()

    def mods_of(frame):
        level = level_ref[frame]
        return lambda kind: mods[kind, pl.ds(level, 1), :]

    def out_copy(place, part):
        target = place * span + part
        return target, pltpu.make_async_remote_copy(
            src_ref=outgoing.at[place, pl.ds(pl.multiple_of(part * rows, rows), rows), :],
            dst_ref=out_ref.at[my_head],
            send_sem=out_send.at[target],
            recv_sem=out_recv,
            device_id={"frame": target, "segment": nxt},
            device_id_type=pl.DeviceIdType.MESH,
        )

    def send_place(place, begin):
        def step(part, carry):
            target, copy = out_copy(place, part)
            remote = jnp.logical_or(target != me, nxt != segment)

            @pl.when(remote)
            def _():
                if begin:
                    copy.start()
                else:
                    copy.wait_send()

            if begin:
                @pl.when(jnp.logical_not(remote))
                def _():
                    pltpu.make_async_copy(
                        outgoing.at[place, pl.ds(pl.multiple_of(part * rows, rows), rows), :],
                        out_ref.at[my_head],
                        out_recv,
                    ).start()

            return carry

        lax.fori_loop(0, span, step, 0)

    @pl.when(owner)
    def _():
        values[:, HEAD:] = jnp.ones((frames * FRAME_TOK, HEAD), jnp.bfloat16)
        pltpu.make_async_copy(
            mod_ref.at[0, :, :, pl.ds(my_columns, HEAD)], mods, mod_sem
        ).wait()
        for frame in range(frames):
            pltpu.make_async_copy(
                gathered.at[frame], gathered.at[frame], state_recv.at[frame]
            ).wait()
            arrived = scales.at[pl.ds(frame * span, span)]
            pltpu.make_async_copy(arrived, arrived, scale_recv.at[frame]).wait()
            row_mods = mods_of(frame)
            for part in range(span):
                column = jnp.sum(
                    jnp.where(diagonal, scales[frame * span + part], 0.0),
                    axis=1,
                    keepdims=True,
                )
                inner = slice(part * rows, (part + 1) * rows)
                outer = slice(frame * FRAME_TOK + part * rows, frame * FRAME_TOK + (part + 1) * rows)
                scaled = (
                    gathered[frame, inner, :].astype(jnp.float32) * column
                ).astype(jnp.bfloat16)
                normed[frame, inner, :] = scaled
                wide = scaled.astype(jnp.float32)
                keys[outer, :] = (
                    wide * (1.0 + row_mods(2)) + row_mods(3)
                ).astype(jnp.bfloat16)
                values[outer, :HEAD] = (
                    wide * (1.0 + row_mods(4)) + row_mods(5)
                ).astype(jnp.bfloat16)

        shift = jnp.where(segment == segments - 1, offset_ref[0], 0)
        for place in range(frames):
            frame = lax.rem(place + shift, frames)
            row_mods = mods_of(frame)
            queries = (
                normed[frame].astype(jnp.float32) * (1.0 + row_mods(0)) + row_mods(1)
            ).astype(jnp.bfloat16)
            bias = jnp.concatenate(
                [
                    jnp.full(
                        (1, FRAME_TOK),
                        jnp.where(mask_ref[frame, other] == 1, 0.0, negative),
                        jnp.float32,
                    )
                    for other in range(frames)
                ],
                axis=1,
            )
            scores = lax.dot_general(
                queries,
                keys[...],
                (((1,), (1,)), ((), ())),
                preferred_element_type=jnp.float32,
            )
            scores = scores * (1.0 / math.sqrt(HEAD)) + bias
            weights = jnp.exp(scores - jnp.max(scores, axis=-1, keepdims=True)).astype(
                jnp.bfloat16
            )
            summed = jnp.dot(weights, values[...], preferred_element_type=jnp.float32)
            attention = (summed[:, :HEAD] / summed[:, HEAD:]).astype(jnp.bfloat16)
            outgoing[place] = (
                gathered[frame].astype(jnp.float32)
                + row_mods(6) * attention.astype(jnp.float32)
            ).astype(jnp.bfloat16)
            send_place(place, True)

    for_heads(end_rows)

    @pl.when(owner)
    def _():
        for place in range(frames):
            send_place(place, False)

    pltpu.make_async_copy(out_ref, out_ref, out_recv).wait()


def body(state, modulation, noise_level, frame_mask, offset):
    _, rows, width = state.shape
    _, levels, kinds, _ = modulation.shape
    devices = lax.axis_size("frame")
    segments = lax.axis_size("segment")
    heads = width // HEAD
    frames = devices * rows // FRAME_TOK
    tokens = devices * rows
    smem = pl.BlockSpec(memory_space=pltpu.SMEM)
    hbm = pl.BlockSpec(memory_space=pl.ANY)
    tiles = pl.pallas_call(
        functools.partial(kernel, devices, segments, heads, frames, rows),
        out_shape=pltpu.VMEM((heads, rows, HEAD), jnp.bfloat16),
        in_specs=[smem, smem, smem, hbm, hbm],
        out_specs=pl.BlockSpec(memory_space=pltpu.VMEM),
        scratch_shapes=[
            pltpu.VMEM((rows, width), jnp.bfloat16),
            pltpu.VMEM((frames, FRAME_TOK, HEAD), jnp.bfloat16),
            pltpu.VMEM((1, HEAD), jnp.float32),
            pltpu.VMEM((devices, 1, HEAD), jnp.float32),
            pltpu.VMEM((kinds, levels, HEAD), jnp.float32),
            pltpu.VMEM((frames, FRAME_TOK, HEAD), jnp.bfloat16),
            pltpu.VMEM((tokens, HEAD), jnp.bfloat16),
            pltpu.VMEM((tokens, 2 * HEAD), jnp.bfloat16),
            pltpu.VMEM((frames, FRAME_TOK, HEAD), jnp.bfloat16),
            pltpu.SemaphoreType.DMA,
            pltpu.SemaphoreType.DMA,
            pltpu.SemaphoreType.DMA((heads,)),
            pltpu.SemaphoreType.DMA((frames,)),
            pltpu.SemaphoreType.DMA((heads,)),
            pltpu.SemaphoreType.DMA((frames,)),
            pltpu.SemaphoreType.DMA((devices,)),
            pltpu.SemaphoreType.DMA,
        ],
        compiler_params=pltpu.CompilerParams(has_side_effects=True, collective_id=0),
        name="denoise",
    )(noise_level, frame_mask, offset, state, jnp.swapaxes(modulation, 1, 2))
    return jnp.swapaxes(tiles, 0, 1).reshape(state.shape)


def solution(mesh):
    return jax.shard_map(
        body,
        mesh=mesh,
        in_specs=(P("segment", "frame", None), P("segment", None, None, None), P(), P(), P()),
        out_specs=P("segment", "frame", None),
        check_vma=False,
    )
```

```python
import functools
import math

import jax
import jax.numpy as jnp
from jax import lax
from jax.experimental import pallas as pl
from jax.experimental.pallas import tpu as pltpu
from jax.sharding import PartitionSpec as P

HEAD = 128
FRAME_TOK = 256

epsilon = 1e-06
negative = -1e30


def kernel(
    devices,
    segments,
    heads,
    frames,
    rows,
    level_ref,
    mask_ref,
    offset_ref,
    state_ref,
    mod_ref,
    out_ref,
    local,
    gathered,
    scale_out,
    scales,
    mods,
    normed,
    keys,
    values,
    outgoing,
    local_sem,
    mod_sem,
    state_send,
    state_recv,
    scale_send,
    scale_recv,
    out_send,
    out_recv,
):
    me = lax.axis_index("frame")
    segment = lax.axis_index("segment")
    span = FRAME_TOK // rows
    width = heads * HEAD
    def owner_of(head):
        return lax.div(head * devices, heads)

    my_head = lax.min(lax.div(me * heads + devices - 1, devices), heads - 1)
    owner = owner_of(my_head) == me
    group = max(heads * span // devices, 1)
    group = group if heads % group == 0 else 1
    my_columns = pl.multiple_of(my_head * HEAD, HEAD)
    my_frame = lax.div(me, span)
    my_row = pl.multiple_of(lax.rem(me, span) * rows, rows)

    nxt = lax.rem(segment + 1, segments)
    barrier = pltpu.get_barrier_semaphore()

    def greet(peer, peer_segment):
        pl.semaphore_signal(
            barrier,
            inc=1,
            device_id={"frame": peer, "segment": peer_segment},
            device_id_type=pl.DeviceIdType.MESH,
        )

    def greet_reader(index, carry):
        greet(lax.rem(me + index, devices), segment)
        return carry

    def greet_writer(head, carry):
        greet(owner_of(head), lax.rem(segment + segments - 1, segments))
        return carry

    fetch = pltpu.make_async_copy(state_ref.at[0], local, local_sem)
    fetch.start()

    @pl.when(owner)
    def _():
        lax.fori_loop(1, devices, greet_reader, 0)
        pltpu.make_async_copy(
            mod_ref.at[0, :, :, pl.ds(my_columns, HEAD)], mods, mod_sem
        ).start()

    if segments > 1:
        lax.fori_loop(0, heads, greet_writer, 0)

    fetch.wait()
    greetings = heads - jnp.where(owner, 1, 0)
    if segments > 1:
        greetings += jnp.where(owner, devices, 0)
    pl.semaphore_wait(barrier, greetings)

    def state_copy(head):
        columns = pl.ds(pl.multiple_of(head * HEAD, HEAD), HEAD)
        return pltpu.make_async_remote_copy(
            src_ref=local.at[:, columns],
            dst_ref=gathered.at[my_frame, pl.ds(my_row, rows), :],
            send_sem=state_send.at[head],
            recv_sem=state_recv.at[my_frame],
            device_id={"frame": owner_of(head)},
            device_id_type=pl.DeviceIdType.MESH,
        )

    def scale_copy(head):
        return pltpu.make_async_remote_copy(
            src_ref=scale_out,
            dst_ref=scales.at[me],
            send_sem=scale_send.at[head],
            recv_sem=scale_recv.at[my_frame],
            device_id={"frame": owner_of(head)},
            device_id_type=pl.DeviceIdType.MESH,
        )

    def for_heads(act):
        def step(index, carry):
            turned = index - lax.rem(index, group) + lax.rem(index + me, group)
            head = lax.rem(lax.div(me * heads, devices) + index, heads)

            @pl.when(owner_of(head) != me)
            def _():
                act(head)

            return carry

        lax.fori_loop(0, heads, step, 0)

    def end_rows(head):
        state_copy(head).wait_send()
        scale_copy(head).wait_send()

    for_heads(lambda head: state_copy(head).start())

    @pl.when(owner)
    def _():
        pltpu.make_async_copy(
            local.at[:, pl.ds(my_columns, HEAD)],
            gathered.at[my_frame, pl.ds(my_row, rows), :],
            state_recv.at[my_frame],
        ).start()

    widened = local[...].astype(jnp.float32)
    square_mean = jnp.sum(widened * widened, axis=-1, keepdims=True) * (1.0 / width)
    factor = lax.rsqrt(square_mean + epsilon)
    diagonal = lax.broadcasted_iota(jnp.int32, (rows, HEAD), 0) == lax.broadcasted_iota(
        jnp.int32, (rows, HEAD), 1
    )
    scale_out[...] = jnp.sum(
        jnp.where(diagonal, factor, 0.0), axis=0, keepdims=True
    )

    for_heads(lambda head: scale_copy(head).start())

    @pl.when(owner)
    def _():
        pltpu.make_async_copy(scale_out, scales.at[me], scale_recv.at[my_frame]).start()

    def mods_of(frame):
        level = level_ref[frame]
        return lambda kind: mods[kind, pl.ds(level, 1), :]

    def out_copy(place, part):
        target = place * span + part
        return target, pltpu.make_async_remote_copy(
            src_ref=outgoing.at[place, pl.ds(pl.multiple_of(part * rows, rows), rows), :],
            dst_ref=out_ref.at[my_head],
            send_sem=out_send.at[target],
            recv_sem=out_recv,
            device_id={"frame": target, "segment": nxt},
            device_id_type=pl.DeviceIdType.MESH,
        )

    def send_place(place, begin):
        def step(part, carry):
            target, copy = out_copy(place, part)
            remote = jnp.logical_or(target != me, nxt != segment)

            @pl.when(remote)
            def _():
                if begin:
                    copy.start()
                else:
                    copy.wait_send()

            if begin:
                @pl.when(jnp.logical_not(remote))
                def _():
                    pltpu.make_async_copy(
                        outgoing.at[place, pl.ds(pl.multiple_of(part * rows, rows), rows), :],
                        out_ref.at[my_head],
                        out_recv,
                    ).start()

            return carry

        lax.fori_loop(0, span, step, 0)

    @pl.when(owner)
    def _():
        values[:, HEAD:] = jnp.ones((frames * FRAME_TOK, HEAD), jnp.bfloat16)
        pltpu.make_async_copy(
            mod_ref.at[0, :, :, pl.ds(my_columns, HEAD)], mods, mod_sem
        ).wait()
        for frame in range(frames):
            pltpu.make_async_copy(
                gathered.at[frame], gathered.at[frame], state_recv.at[frame]
            ).wait()
            arrived = scales.at[pl.ds(frame * span, span)]
            pltpu.make_async_copy(arrived, arrived, scale_recv.at[frame]).wait()
            row_mods = mods_of(frame)
            for part in range(span):
                column = jnp.sum(
                    jnp.where(diagonal, scales[frame * span + part], 0.0),
                    axis=1,
                    keepdims=True,
                )
                inner = slice(part * rows, (part + 1) * rows)
                outer = slice(frame * FRAME_TOK + part * rows, frame * FRAME_TOK + (part + 1) * rows)
                scaled = (
                    gathered[frame, inner, :].astype(jnp.float32) * column
                ).astype(jnp.bfloat16)
                normed[frame, inner, :] = scaled
                wide = scaled.astype(jnp.float32)
                keys[outer, :] = (
                    wide * (1.0 + row_mods(2)) + row_mods(3)
                ).astype(jnp.bfloat16)
                values[outer, :HEAD] = (
                    wide * (1.0 + row_mods(4)) + row_mods(5)
                ).astype(jnp.bfloat16)

        shift = jnp.where(segment == segments - 1, offset_ref[0], 0)
        for turn in range(frames):
            place = jnp.where(2 * me >= devices, turn, (frames - turn) % frames)
            frame = lax.rem(place + shift, frames)
            row_mods = mods_of(frame)
            queries = (
                normed[frame].astype(jnp.float32) * (1.0 + row_mods(0)) + row_mods(1)
            ).astype(jnp.bfloat16)
            bias = jnp.concatenate(
                [
                    jnp.full(
                        (1, FRAME_TOK),
                        jnp.where(mask_ref[frame, other] == 1, 0.0, negative),
                        jnp.float32,
                    )
                    for other in range(frames)
                ],
                axis=1,
            )
            scores = lax.dot_general(
                queries,
                keys[...],
                (((1,), (1,)), ((), ())),
                preferred_element_type=jnp.float32,
            )
            scores = scores * (1.0 / math.sqrt(HEAD)) + bias
            weights = jnp.exp(scores - jnp.max(scores, axis=-1, keepdims=True)).astype(
                jnp.bfloat16
            )
            summed = jnp.dot(weights, values[...], preferred_element_type=jnp.float32)
            attention = (summed[:, :HEAD] / summed[:, HEAD:]).astype(jnp.bfloat16)
            outgoing[place] = (
                gathered[frame].astype(jnp.float32)
                + row_mods(6) * attention.astype(jnp.float32)
            ).astype(jnp.bfloat16)
            send_place(place, True)

    for_heads(end_rows)

    @pl.when(owner)
    def _():
        for place in range(frames):
            send_place(place, False)

    pltpu.make_async_copy(out_ref, out_ref, out_recv).wait()


def body(state, modulation, noise_level, frame_mask, offset):
    _, rows, width = state.shape
    _, levels, kinds, _ = modulation.shape
    devices = lax.axis_size("frame")
    segments = lax.axis_size("segment")
    heads = width // HEAD
    frames = devices * rows // FRAME_TOK
    tokens = devices * rows
    smem = pl.BlockSpec(memory_space=pltpu.SMEM)
    hbm = pl.BlockSpec(memory_space=pl.ANY)
    tiles = pl.pallas_call(
        functools.partial(kernel, devices, segments, heads, frames, rows),
        out_shape=pltpu.VMEM((heads, rows, HEAD), jnp.bfloat16),
        in_specs=[smem, smem, smem, hbm, hbm],
        out_specs=pl.BlockSpec(memory_space=pltpu.VMEM),
        scratch_shapes=[
            pltpu.VMEM((rows, width), jnp.bfloat16),
            pltpu.VMEM((frames, FRAME_TOK, HEAD), jnp.bfloat16),
            pltpu.VMEM((1, HEAD), jnp.float32),
            pltpu.VMEM((devices, 1, HEAD), jnp.float32),
            pltpu.VMEM((kinds, levels, HEAD), jnp.float32),
            pltpu.VMEM((frames, FRAME_TOK, HEAD), jnp.bfloat16),
            pltpu.VMEM((tokens, HEAD), jnp.bfloat16),
            pltpu.VMEM((tokens, 2 * HEAD), jnp.bfloat16),
            pltpu.VMEM((frames, FRAME_TOK, HEAD), jnp.bfloat16),
            pltpu.SemaphoreType.DMA,
            pltpu.SemaphoreType.DMA,
            pltpu.SemaphoreType.DMA((heads,)),
            pltpu.SemaphoreType.DMA((frames,)),
            pltpu.SemaphoreType.DMA((heads,)),
            pltpu.SemaphoreType.DMA((frames,)),
            pltpu.SemaphoreType.DMA((devices,)),
            pltpu.SemaphoreType.DMA,
        ],
        compiler_params=pltpu.CompilerParams(has_side_effects=True, collective_id=0),
        name="denoise",
    )(noise_level, frame_mask, offset, state, jnp.swapaxes(modulation, 1, 2))
    return jnp.swapaxes(tiles, 0, 1).reshape(state.shape)


def solution(mesh):
    return jax.shard_map(
        body,
        mesh=mesh,
        in_specs=(P("segment", "frame", None), P("segment", None, None, None), P(), P(), P()),
        out_specs=P("segment", "frame", None),
        check_vma=False,
    )
```

```python
import functools
import math

import jax
import jax.numpy as jnp
from jax import lax
from jax.experimental import pallas as pl
from jax.experimental.pallas import tpu as pltpu
from jax.sharding import PartitionSpec as P

HEAD = 128
FRAME_TOK = 256

epsilon = 1e-06
negative = -1e30


def kernel(
    devices,
    segments,
    heads,
    frames,
    rows,
    level_ref,
    mask_ref,
    offset_ref,
    state_ref,
    mod_ref,
    out_ref,
    local,
    gathered,
    scale_out,
    scales,
    mods,
    normed,
    keys,
    values,
    outgoing,
    local_sem,
    mod_sem,
    state_send,
    state_recv,
    scale_send,
    scale_recv,
    out_send,
    out_recv,
):
    me = lax.axis_index("frame")
    segment = lax.axis_index("segment")
    span = FRAME_TOK // rows
    width = heads * HEAD
    half = span // math.gcd(span, 2)
    def owner_of(head):
        return lax.div(head * devices, heads)

    my_head = lax.min(lax.div(me * heads + devices - 1, devices), heads - 1)
    owner = owner_of(my_head) == me
    group = max(heads * span // devices, 1)
    group = group if heads % group == 0 else 1
    my_columns = pl.multiple_of(my_head * HEAD, HEAD)
    my_frame = lax.div(me, span)
    my_row = pl.multiple_of(lax.rem(me, span) * rows, rows)

    nxt = lax.rem(segment + 1, segments)
    barrier = pltpu.get_barrier_semaphore()

    def greet(peer, peer_segment):
        pl.semaphore_signal(
            barrier,
            inc=1,
            device_id={"frame": peer, "segment": peer_segment},
            device_id_type=pl.DeviceIdType.MESH,
        )

    def greet_reader(index, carry):
        greet(lax.rem(me + index, devices), segment)
        return carry

    def greet_writer(head, carry):
        greet(owner_of(head), lax.rem(segment + segments - 1, segments))
        return carry

    fetch = pltpu.make_async_copy(state_ref.at[0], local, local_sem)
    fetch.start()

    @pl.when(owner)
    def _():
        lax.fori_loop(1, devices, greet_reader, 0)
        pltpu.make_async_copy(
            mod_ref.at[0, :, :, pl.ds(my_columns, HEAD)], mods, mod_sem
        ).start()

    if segments > 1:
        lax.fori_loop(0, heads, greet_writer, 0)

    fetch.wait()
    greetings = heads - jnp.where(owner, 1, 0)
    if segments > 1:
        greetings += jnp.where(owner, devices, 0)
    pl.semaphore_wait(barrier, greetings)

    def state_copy(head):
        columns = pl.ds(pl.multiple_of(head * HEAD, HEAD), HEAD)
        return pltpu.make_async_remote_copy(
            src_ref=local.at[:, columns],
            dst_ref=gathered.at[my_frame, pl.ds(my_row, rows), :],
            send_sem=state_send.at[head],
            recv_sem=state_recv.at[my_frame],
            device_id={"frame": owner_of(head)},
            device_id_type=pl.DeviceIdType.MESH,
        )

    def scale_copy(head):
        return pltpu.make_async_remote_copy(
            src_ref=scale_out,
            dst_ref=scales.at[me],
            send_sem=scale_send.at[head],
            recv_sem=scale_recv.at[my_frame],
            device_id={"frame": owner_of(head)},
            device_id_type=pl.DeviceIdType.MESH,
        )

    def for_heads(act):
        def step(index, carry):
            turned = index - lax.rem(index, group) + lax.rem(index + me, group)
            head = lax.rem(lax.div(me * heads, devices) + index, heads)

            @pl.when(owner_of(head) != me)
            def _():
                act(head)

            return carry

        lax.fori_loop(0, heads, step, 0)

    def end_rows(head):
        state_copy(head).wait_send()
        scale_copy(head).wait_send()

    for_heads(lambda head: state_copy(head).start())

    @pl.when(owner)
    def _():
        pltpu.make_async_copy(
            local.at[:, pl.ds(my_columns, HEAD)],
            gathered.at[my_frame, pl.ds(my_row, rows), :],
            state_recv.at[my_frame],
        ).start()

    widened = local[...].astype(jnp.float32)
    square_mean = jnp.sum(widened * widened, axis=-1, keepdims=True) * (1.0 / width)
    factor = lax.rsqrt(square_mean + epsilon)
    diagonal = lax.broadcasted_iota(jnp.int32, (rows, HEAD), 0) == lax.broadcasted_iota(
        jnp.int32, (rows, HEAD), 1
    )
    scale_out[...] = jnp.sum(
        jnp.where(diagonal, factor, 0.0), axis=0, keepdims=True
    )

    for_heads(lambda head: scale_copy(head).start())

    @pl.when(owner)
    def _():
        pltpu.make_async_copy(scale_out, scales.at[me], scale_recv.at[my_frame]).start()

    def mods_of(frame):
        level = level_ref[frame]
        return lambda kind: mods[kind, pl.ds(level, 1), :]

    def out_copy(place, part):
        target = place * span + part
        return target, pltpu.make_async_remote_copy(
            src_ref=outgoing.at[place, pl.ds(pl.multiple_of(part * rows, rows), rows), :],
            dst_ref=out_ref.at[my_head],
            send_sem=out_send.at[target],
            recv_sem=out_recv,
            device_id={"frame": target, "segment": nxt},
            device_id_type=pl.DeviceIdType.MESH,
        )

    def send_place(place, begin, first, last):
        def step(part, carry):
            target, copy = out_copy(place, part)
            remote = jnp.logical_or(target != me, nxt != segment)

            @pl.when(remote)
            def _():
                if begin:
                    copy.start()
                else:
                    copy.wait_send()

            if begin:
                @pl.when(jnp.logical_not(remote))
                def _():
                    pltpu.make_async_copy(
                        outgoing.at[place, pl.ds(pl.multiple_of(part * rows, rows), rows), :],
                        out_ref.at[my_head],
                        out_recv,
                    ).start()

            return carry

        lax.fori_loop(first, last, step, 0)

    @pl.when(owner)
    def _():
        values[:, HEAD:] = jnp.ones((frames * FRAME_TOK, HEAD), jnp.bfloat16)
        pltpu.make_async_copy(
            mod_ref.at[0, :, :, pl.ds(my_columns, HEAD)], mods, mod_sem
        ).wait()
        for frame in range(frames):
            pltpu.make_async_copy(
                gathered.at[frame], gathered.at[frame], state_recv.at[frame]
            ).wait()
            arrived = scales.at[pl.ds(frame * span, span)]
            pltpu.make_async_copy(arrived, arrived, scale_recv.at[frame]).wait()
            row_mods = mods_of(frame)
            for part in range(span):
                column = jnp.sum(
                    jnp.where(diagonal, scales[frame * span + part], 0.0),
                    axis=1,
                    keepdims=True,
                )
                inner = slice(part * rows, (part + 1) * rows)
                outer = slice(frame * FRAME_TOK + part * rows, frame * FRAME_TOK + (part + 1) * rows)
                scaled = (
                    gathered[frame, inner, :].astype(jnp.float32) * column
                ).astype(jnp.bfloat16)
                normed[frame, inner, :] = scaled
                wide = scaled.astype(jnp.float32)
                keys[outer, :] = (
                    wide * (1.0 + row_mods(2)) + row_mods(3)
                ).astype(jnp.bfloat16)
                values[outer, :HEAD] = (
                    wide * (1.0 + row_mods(4)) + row_mods(5)
                ).astype(jnp.bfloat16)

        shift = jnp.where(segment == segments - 1, offset_ref[0], 0)
        for turn in range(frames):
            place = jnp.where(2 * me >= devices, turn, (frames - turn) % frames)
            frame = lax.rem(place + shift, frames)
            row_mods = mods_of(frame)
            bias = jnp.concatenate(
                [
                    jnp.full(
                        (1, FRAME_TOK),
                        jnp.where(mask_ref[frame, other] == 1, 0.0, negative),
                        jnp.float32,
                    )
                    for other in range(frames)
                ],
                axis=1,
            )
            for first in range(0, span, half):
                inner = slice(first * rows, (first + half) * rows)
                queries = (
                    normed[frame, inner, :].astype(jnp.float32) * (1.0 + row_mods(0)) + row_mods(1)
                ).astype(jnp.bfloat16)
                scores = lax.dot_general(
                    queries,
                    keys[...],
                    (((1,), (1,)), ((), ())),
                    preferred_element_type=jnp.float32,
                )
                scores = scores * (1.0 / math.sqrt(HEAD)) + bias
                weights = jnp.exp(scores - jnp.max(scores, axis=-1, keepdims=True)).astype(
                    jnp.bfloat16
                )
                summed = jnp.dot(weights, values[...], preferred_element_type=jnp.float32)
                attention = (summed[:, :HEAD] / summed[:, HEAD:]).astype(jnp.bfloat16)
                outgoing[place, inner, :] = (
                    gathered[frame, inner, :].astype(jnp.float32)
                    + row_mods(6) * attention.astype(jnp.float32)
                ).astype(jnp.bfloat16)
                send_place(place, True, first, first + half)

    for_heads(end_rows)

    @pl.when(owner)
    def _():
        for place in range(frames):
            send_place(place, False, 0, span)

    pltpu.make_async_copy(out_ref, out_ref, out_recv).wait()


def body(state, modulation, noise_level, frame_mask, offset):
    _, rows, width = state.shape
    _, levels, kinds, _ = modulation.shape
    devices = lax.axis_size("frame")
    segments = lax.axis_size("segment")
    heads = width // HEAD
    frames = devices * rows // FRAME_TOK
    tokens = devices * rows
    smem = pl.BlockSpec(memory_space=pltpu.SMEM)
    hbm = pl.BlockSpec(memory_space=pl.ANY)
    tiles = pl.pallas_call(
        functools.partial(kernel, devices, segments, heads, frames, rows),
        out_shape=pltpu.VMEM((heads, rows, HEAD), jnp.bfloat16),
        in_specs=[smem, smem, smem, hbm, hbm],
        out_specs=pl.BlockSpec(memory_space=pltpu.VMEM),
        scratch_shapes=[
            pltpu.VMEM((rows, width), jnp.bfloat16),
            pltpu.VMEM((frames, FRAME_TOK, HEAD), jnp.bfloat16),
            pltpu.VMEM((1, HEAD), jnp.float32),
            pltpu.VMEM((devices, 1, HEAD), jnp.float32),
            pltpu.VMEM((kinds, levels, HEAD), jnp.float32),
            pltpu.VMEM((frames, FRAME_TOK, HEAD), jnp.bfloat16),
            pltpu.VMEM((tokens, HEAD), jnp.bfloat16),
            pltpu.VMEM((tokens, 2 * HEAD), jnp.bfloat16),
            pltpu.VMEM((frames, FRAME_TOK, HEAD), jnp.bfloat16),
            pltpu.SemaphoreType.DMA,
            pltpu.SemaphoreType.DMA,
            pltpu.SemaphoreType.DMA((heads,)),
            pltpu.SemaphoreType.DMA((frames,)),
            pltpu.SemaphoreType.DMA((heads,)),
            pltpu.SemaphoreType.DMA((frames,)),
            pltpu.SemaphoreType.DMA((devices,)),
            pltpu.SemaphoreType.DMA,
        ],
        compiler_params=pltpu.CompilerParams(has_side_effects=True, collective_id=0),
        name="denoise",
    )(noise_level, frame_mask, offset, state, jnp.swapaxes(modulation, 1, 2))
    return jnp.swapaxes(tiles, 0, 1).reshape(state.shape)


def solution(mesh):
    return jax.shard_map(
        body,
        mesh=mesh,
        in_specs=(P("segment", "frame", None), P("segment", None, None, None), P(), P(), P()),
        out_specs=P("segment", "frame", None),
        check_vma=False,
    )
```
